32 devices in a mesh: dp: 8 (over y, x, core), seq: 4 (over z).
Axes of the slice: x: 2, y: 2, z: 4, core: 2. Of those that a mesh axis runs over, the one named last changes fastest.
Arguments:
- query_rows: bfloat16 [8, 512, 3072], P('dp', 'seq'), may hold values from -6 to 6
- key_rows: bfloat16 [8, 512, 3072], P('dp', 'seq'), may hold values from -6 to 6
- value_rows: bfloat16 [8, 512, 3072], P('dp', 'seq'), may hold values from -6 to 6
- out_grad: bfloat16 [8, 512, 6144], P('dp', 'seq'), may hold values from -54 to 54
- clip_lengths: int32 [8, 4], P('dp'), may hold values from 1 to 256, 512 in all within a row
- out_weight: bfloat16 [3072, 6144], P('seq'), may hold values from -0.109375 to 0.109375
- query_gain: float32 [128], replicated, may hold values from 0.1 to 1.9
- key_gain: float32 [128], replicated, may hold values from 0.1 to 1.9
Outputs:
- query_grad: bfloat16 [8, 512, 3072], P('dp', 'seq')
- key_grad: bfloat16 [8, 512, 3072], P('dp', 'seq')
- value_grad: bfloat16 [8, 512, 3072], P('dp', 'seq')
- weight_grad: float32 [3072, 6144], P('seq', 'dp')
- querygain_grad: float32 [128], replicated
- keygain_grad: float32 [128], replicated
- grad_norm: float32 [], replicated
The draws below stay inside these ranges and needn't reach their ends.
Inputs may be any that keep to these rules, and one draw needn't show every extreme that they name: `clip_lengths`: the token counts of each group's clips sum to 512.
All inputs are finite; a program needn't handle non-finite values.
Results may differ from the reference program's by a relative error of at most 0.015.
Values may be sent and summed in bfloat16 or wider, within the bound.
No kernel may reach another device: no remote copies, remote signals or barrier semaphores. Data moves between devices by JAX's collectives and lax.ppermute only.
A program may use at most 128 MiB of HBM per device.

```python
import math
import jax
import jax.numpy as jnp
import numpy as np
from jax import lax

D = 6144
HEAD_DIM = 128
CLIPS = 4
GROUPS = 8
SEQ_LEN = 512
INNER = 3072
MAX_NORM = 768


def draw_out_grad(key, part):
    first = jax.random.fold_in(key, 0)
    second = jax.random.fold_in(key, 1)
    fifth = jax.random.fold_in(key, 4)
    row_scale = jnp.exp(jax.random.uniform(first, (GROUPS, SEQ_LEN, 1), jnp.float32, -1.2, 1.1))
    ramp = 0.5 + jnp.arange(D, dtype=jnp.float32) / (D - 1)
    column_scale = ramp * jnp.exp(jax.random.uniform(second, (D,), jnp.float32, -1.2, 1.1))
    base = jax.random.truncated_normal(fifth, -4.0, 4.0, (GROUPS, SEQ_LEN, D), jnp.float32)
    return (row_scale * column_scale * base).astype(jnp.bfloat16)


def block_scale(rng, dims, shards, smallest, top_value):
    loudness = 1.0
    for dim, blocks in shards:
        steps = jax.random.uniform(jax.random.fold_in(jax.random.fold_in(rng, 6), dim), (blocks,), jnp.float32, smallest / len(shards), top_value / len(shards))
        loudness = loudness * jnp.repeat(jnp.exp(steps), dims[dim] // blocks).reshape((-1,) + (1,) * (len(dims) - 1 - dim))
    return loudness


def length_profile(number_of, total, most, lean):
    loads = [(1 << 20) // math.isqrt(standing ** lean) + 1 for standing in range(2, number_of + 1)]
    rest, holding = total - most - (number_of - 1), [1] * (number_of - 1)
    while rest > 0:
        free = [i for i in range(number_of - 1) if holding[i] < most]
        pool, remaining = sum([loads[i] for i in free]), rest
        for i in free:
            addition = min(most - holding[i], max(1, remaining * loads[i] // pool), rest)
            holding[i] = holding[i] + addition
            rest = rest - addition
    return np.array([most] + holding)


def ragged_sizes(own_key, amount, total, bound, slope):
    if amount == 2:
        one = jax.random.randint(own_key, (), max(1, total - bound), min(bound, total - 1) + 1)
        return jnp.stack([one, total - one])
    sizes = jnp.asarray(length_profile(amount, total, bound, slope), jnp.int32)
    couples = (amount - 1) // 2
    giver, receiver = sizes[1:1 + 2 * couples:2], sizes[2:2 + 2 * couples:2]
    room = jnp.minimum(giver - 1, bound - receiver)
    passed = jax.random.randint(jax.random.fold_in(own_key, 1), (couples,), 0, 1 << 20) % (room + 1)
    sizes = sizes.at[1:1 + 2 * couples:2].set(giver - passed).at[2:2 + 2 * couples:2].set(receiver + passed)
    return sizes[jax.random.permutation(jax.random.fold_in(own_key, 2), amount)]


def bell_draw(own_key, shape, scale, limit, cuts=(), held_as=jnp.bfloat16):
    values = jax.random.normal(own_key, shape, jnp.float32) * scale
    if len(cuts) > 0:
        values = block_scale(own_key, shape, cuts, -0.22, 0.18) * values
    return jnp.clip(values, min=-limit, max=limit).astype(held_as)


def setup_inputs(seed: int = 0) -> dict:
    splits = jax.random.split(jax.random.key(seed), 9)
    return {
        "query_rows": bell_draw(splits[0], (GROUPS, SEQ_LEN, INNER), 1.0, 6.0, ((0, 8), (1, 4))),
        "key_rows": bell_draw(splits[1], (GROUPS, SEQ_LEN, INNER), 1.0, 6.0, ((0, 8), (1, 4))),
        "value_rows": bell_draw(splits[2], (GROUPS, SEQ_LEN, INNER), 1.0, 6.0, ((0, 8), (1, 4))),
        "out_grad": draw_out_grad(jax.random.fold_in(splits[8], 71), 0),
        "clip_lengths": jax.vmap(lambda own: ragged_sizes(own, CLIPS, SEQ_LEN, SEQ_LEN // 2, 2))(jax.random.split(splits[4], GROUPS)).reshape((GROUPS, CLIPS)).astype(jnp.int32),
        "out_weight": bell_draw(splits[5], (INNER, D), INNER ** -0.5, 0.109375, ((0, 4),)),
        "query_gain": jnp.clip(1.0 + 0.18 * jax.random.normal(splits[6], (HEAD_DIM,), jnp.float32), 0.1, 1.9),
        "key_gain": jnp.clip(1.0 + 0.18 * jax.random.normal(splits[7], (HEAD_DIM,), jnp.float32), 0.1, 1.9),
    }


EPS = 1e-06

def segment_ids(lengths, total):
    ends = jnp.cumsum(lengths.astype(jnp.int32))
    places = jnp.arange(total, dtype=jnp.int32)
    return lax.optimization_barrier(jnp.sum((places[:, None] >= ends[None, :]).astype(jnp.int32), axis=1)).astype(jnp.int32)

def norm_rows(rows, gain):
    wide = rows.astype(jnp.float32)
    inverse = lax.rsqrt(lax.optimization_barrier(jnp.mean(wide * wide, axis=-1, keepdims=True)) + EPS)
    unit = wide * inverse
    return (unit, inverse, (unit * gain).astype(jnp.bfloat16))

def norm_back(unit, inverse, gain, d_norm):
    gain_part = lax.optimization_barrier(jnp.sum(unit * d_norm, axis=(0, 1)))
    d_unit = d_norm * gain
    d_rows = inverse * (d_unit - unit * lax.optimization_barrier(jnp.mean(unit * d_unit, axis=-1, keepdims=True)))
    return (d_rows.astype(jnp.bfloat16), gain_part)

def one_group(query, keys, values, d_out, lengths, out_weight, query_gain, key_gain):
    total = query.shape[0]
    heads = query.shape[1] // HEAD_DIM
    scale = HEAD_DIM ** (-0.5)
    query3 = query.reshape(total, heads, HEAD_DIM)
    keys3 = keys.reshape(total, heads, HEAD_DIM)
    values3 = values.reshape(total, heads, HEAD_DIM).astype(jnp.float32)
    seg = segment_ids(lengths, total)
    same = seg[:, None] == seg[None, :]
    q_unit, q_inv, q_norm = norm_rows(query3, query_gain)
    k_unit, k_inv, k_norm = norm_rows(keys3, key_gain)
    scores = jnp.einsum('qhd,khd->hqk', q_norm.astype(jnp.float32), k_norm.astype(jnp.float32)) * scale
    expo = jnp.where(same[None], jnp.exp(scores), 0.0)
    probs = (expo / lax.optimization_barrier(jnp.sum(expo, axis=-1, keepdims=True))).astype(jnp.bfloat16)
    probs32 = probs.astype(jnp.float32)
    attn_out = jnp.einsum('hqk,khd->qhd', probs32, values3).astype(jnp.bfloat16)
    attn_flat = attn_out.reshape(total, heads * HEAD_DIM)
    weight_part = jnp.dot(attn_flat.T, d_out, preferred_element_type=jnp.float32)
    d_attn = jnp.dot(d_out, out_weight.T, preferred_element_type=jnp.float32).astype(jnp.bfloat16)
    d_attn32 = d_attn.reshape(total, heads, HEAD_DIM).astype(jnp.float32)
    d_probs = jnp.einsum('qhd,khd->hqk', d_attn32, values3)
    row_sum = lax.optimization_barrier(jnp.sum(probs32 * d_probs, axis=-1, keepdims=True))
    d_scores = (probs32 * (d_probs - row_sum) * scale).astype(jnp.bfloat16).astype(jnp.float32)
    value_grad = jnp.einsum('hqk,qhd->khd', probs32, d_attn32).astype(jnp.bfloat16)
    d_qnorm = jnp.einsum('hqk,khd->qhd', d_scores, k_norm.astype(jnp.float32))
    d_knorm = jnp.einsum('hqk,qhd->khd', d_scores, q_norm.astype(jnp.float32))
    query_grad, q_gain_part = norm_back(q_unit, q_inv, query_gain, d_qnorm)
    key_grad, k_gain_part = norm_back(k_unit, k_inv, key_gain, d_knorm)
    width = heads * HEAD_DIM
    return (query_grad.reshape(total, width), key_grad.reshape(total, width), value_grad.reshape(total, width), weight_part, q_gain_part, k_gain_part)

def reference(query_rows, key_rows, value_rows, out_grad, clip_lengths, out_weight, query_gain, key_gain):

    def step(carry, items):
        weight_sum, q_gain_sum, k_gain_sum = carry
        query, keys, values, d_out, lengths = items
        q_grad, k_grad, v_grad, weight_part, q_part, k_part = one_group(query, keys, values, d_out, lengths, out_weight, query_gain, key_gain)
        return ((weight_sum + weight_part, q_gain_sum + q_part, k_gain_sum + k_part), (q_grad, k_grad, v_grad))
    start = (jnp.zeros(out_weight.shape, jnp.float32), jnp.zeros((HEAD_DIM,), jnp.float32), jnp.zeros((HEAD_DIM,), jnp.float32))
    (weight_raw, qgain_raw, kgain_raw), (query_grad, key_grad, value_grad) = lax.scan(step, start, (query_rows, key_rows, value_rows, out_grad, clip_lengths))
    squares = jnp.sum(weight_raw * weight_raw) + jnp.sum(qgain_raw * qgain_raw) + jnp.sum(kgain_raw * kgain_raw)
    grad_norm = jnp.sqrt(squares)
    factor = jnp.minimum(jnp.float32(1.0), MAX_NORM / (grad_norm + EPS))
    return (query_grad, key_grad, value_grad, weight_raw * factor, qgain_raw * factor, kgain_raw * factor, grad_norm)
```

```python
import functools
import jax
import jax.numpy as jnp
from jax import lax
from jax.experimental import pallas as pl
from jax.experimental.pallas import tpu as pltpu
from jax.sharding import PartitionSpec as P

HEAD_DIM = 128
MAX_NORM = 768
EPS = 1e-06
CORES = 2
CHUNKS = 3
VMEM_BYTES = 60 * 1024 * 1024


ANY = pl.BlockSpec(memory_space=pl.ANY)
SMEM = pl.BlockSpec(memory_space=pltpu.SMEM)
VMEM = pl.BlockSpec(memory_space=pltpu.VMEM)


def run(body, outs, args, in_specs, out_specs, scratch, name):
    return pl.pallas_call(
        body,
        out_shape=outs,
        in_specs=in_specs,
        out_specs=out_specs,
        scratch_shapes=scratch,
        compiler_params=pltpu.CompilerParams(vmem_limit_bytes=VMEM_BYTES),
        name=name,
    )(*args)


def chunk_heads(heads):
    count = min(CHUNKS, heads)
    base, extra = divmod(heads, count)
    return [base + (1 if i < extra else 0) for i in range(count)]


def pack_body(place_ref, *refs, ways, width, chunks):
    rows = refs[:3]
    outs = refs[3:-1]
    sems = refs[-1]
    place = place_ref[0]
    copies = []
    slot = 0
    for start, size in chunks:
        for step in range(ways):
            target = lax.rem(place + step, ways)
            column = pl.multiple_of(target * width + start, 128)
            for which in range(3):
                copies.append(
                    pltpu.make_async_copy(
                        rows[which].at[:, pl.ds(column, size)],
                        outs[slot].at[which],
                        sems.at[len(copies)],
                    )
                )
            slot += 1
    for copy in copies:
        copy.start()
    for copy in copies:
        copy.wait()


def unpack_body(place_ref, *refs, ways, width, chunks):
    count = len(chunks) * ways
    pieces = refs[:count]
    outs = refs[count : count + 3]
    sems = refs[-1]
    place = place_ref[0]
    copies = []
    slot = 0
    for start, size in chunks:
        for step in range(ways):
            source = lax.rem(place + step, ways)
            column = pl.multiple_of(source * width + start, 128)
            for which in range(3):
                copies.append(
                    pltpu.make_async_copy(
                        pieces[slot].at[which],
                        outs[which].at[:, pl.ds(column, size)],
                        sems.at[len(copies)],
                    )
                )
            slot += 1
    for copy in copies:
        copy.start()
    for copy in copies:
        copy.wait()


def d_attn_body(place_ref, *refs, ways, rows, chunks, outer, cols, aligned):
    own, right, left = refs[0], refs[1:ways], refs[ways : 2 * ways - 1]
    weight = refs[2 * ways - 1]
    rest = refs[2 * ways :]
    d_outs = rest[: len(chunks)]
    extra = rest[len(chunks) : len(chunks) + (2 if aligned else 1)]
    full, weight_vmem, sems, out_sems = rest[-4:]
    place = place_ref[0]
    group = place_ref[1]
    load = pltpu.make_async_copy(weight, weight_vmem, sems.at[ways])
    load.start()

    def fetch(step, source):
        return pltpu.make_async_copy(source, full.at[pl.ds(step * rows, rows)], sems.at[step])

    fetch(0, own).start()
    for step in range(1, ways):

        @pl.when(place >= step)
        def _():
            fetch(step, right[step - 1]).start()

        @pl.when(place < step)
        def _():
            fetch(step, left[ways - step - 1]).start()

    load.wait()
    for step in range(ways):
        fetch(step, own).wait()
    writes = []
    if aligned:
        core = lax.rem(group, CORES)
        chip = lax.div(group, CORES)
        for step in range(outer):
            block = lax.bitwise_xor(chip, step) * CORES
            for side in range(2):
                lane = lax.bitwise_xor(core, side)
                column = pl.multiple_of((block + lane) * cols, 128)
                writes.append(
                    pltpu.make_async_copy(
                        full.at[:, pl.ds(column, cols)],
                        extra[side].at[step],
                        out_sems.at[2 * step + side],
                    )
                )
    else:
        writes.append(pltpu.make_async_copy(full, extra[0], out_sems.at[0]))
    for write in writes:
        write.start()
    for index, (start, size) in enumerate(chunks):
        d_outs[index][...] = lax.dot_general(
            full[...],
            weight_vmem[start : start + size, :],
            (((1,), (1,)), ((), ())),
            preferred_element_type=jnp.float32,
        ).astype(jnp.bfloat16)
    for write in writes:
        write.wait()


def attention_body(place_ref, lengths_ref, *refs, ways, rows, heads):
    pieces = refs[:ways]
    d_attn_ref, q_gain_ref, k_gain_ref = refs[ways : ways + 3]
    attn_t_ref, gains_ref = refs[ways + 3], refs[ways + 4]
    outs = refs[ways + 5 : 2 * ways + 5]
    total = ways * rows
    place = place_ref[0]
    q_gain = q_gain_ref[...]
    k_gain = k_gain_ref[...]
    scale = HEAD_DIM ** (-0.5)

    def segments(shape, dim):
        index = lax.broadcasted_iota(jnp.int32, shape, dim)
        step = lax.div(index, rows)
        source = place - step
        source = jnp.where(source < 0, source + ways, source)
        position = source * rows + lax.rem(index, rows)
        seg = jnp.zeros(shape, jnp.int32)
        end = jnp.int32(0)
        for clip in range(lengths_ref.shape[1]):
            end = end + lengths_ref[0, clip]
            seg = seg + (position >= end).astype(jnp.int32)
        return seg

    same = segments((total, 1), 0) == segments((1, total), 1)
    q_sum = jnp.zeros((1, HEAD_DIM), jnp.float32)
    k_sum = jnp.zeros((1, HEAD_DIM), jnp.float32)
    for head in range(heads):
        part = slice(head * HEAD_DIM, (head + 1) * HEAD_DIM)

        def gather(which):
            return jnp.concatenate([piece[which, :, part] for piece in pieces], axis=0)

        def norm(raw, gain):
            wide = raw.astype(jnp.float32)
            inverse = lax.rsqrt(jnp.mean(wide * wide, axis=-1, keepdims=True) + EPS)
            unit = wide * inverse
            return unit, inverse, (unit * gain).astype(jnp.bfloat16)

        q_unit, q_inv, q_norm = norm(gather(0), q_gain)
        k_unit, k_inv, k_norm = norm(gather(1), k_gain)
        value = gather(2)
        d_attn = d_attn_ref[:, part]
        nt = (((1,), (1,)), ((), ()))
        nn = (((1,), (0,)), ((), ()))

        def dot(a, b, dims):
            return lax.dot_general(a, b, dims, preferred_element_type=jnp.float32)

        scores_t = dot(k_norm, q_norm, nt) * scale
        expo = jnp.where(same, jnp.exp(scores_t), 0.0)
        inverse_sum = 1.0 / jnp.sum(expo, axis=0, keepdims=True)
        probs = (expo * inverse_sum).astype(jnp.bfloat16)
        attn_t = dot(value.T, probs, nn)
        attn_t_ref[part, :] = attn_t.astype(jnp.bfloat16)
        d_probs = dot(value, d_attn, nt)
        probs32 = probs.astype(jnp.float32)
        row_sum = jnp.sum(probs32 * d_probs, axis=0, keepdims=True)
        d_scores = (probs32 * (d_probs - row_sum) * scale).astype(jnp.bfloat16)
        d_value = dot(probs, d_attn, nn).astype(jnp.bfloat16)
        d_k = dot(d_scores, q_norm, nn)
        d_q = dot(k_norm.T, d_scores, nn).T

        def back(unit, inverse, gain, d_norm):
            d_unit = d_norm * gain
            grad = inverse * (d_unit - unit * jnp.mean(unit * d_unit, axis=-1, keepdims=True))
            return grad.astype(jnp.bfloat16), jnp.sum(unit * d_norm, axis=0, keepdims=True)

        q_grad, q_part = back(q_unit, q_inv, q_gain, d_q)
        k_grad, k_part = back(k_unit, k_inv, k_gain, d_k)
        q_sum = q_sum + q_part
        k_sum = k_sum + k_part
        for step in range(ways):
            block = slice(step * rows, (step + 1) * rows)
            outs[step][0, :, part] = q_grad[block]
            outs[step][1, :, part] = k_grad[block]
            outs[step][2, :, part] = d_value[block]
    gains_ref[...] = jnp.concatenate(
        [q_sum, k_sum, jnp.zeros((6, HEAD_DIM), jnp.float32)], axis=0
    )


def weight_body(*refs, outer):
    own_t, other_t, mine, theirs = refs[:4]
    outs = refs[4 : 4 + outer]
    mine_vmem, theirs_vmem, sems = refs[4 + outer :]
    copies = []
    for step in range(outer):
        copies.append(pltpu.make_async_copy(mine.at[step], mine_vmem.at[step], sems.at[2 * step]))
        copies.append(
            pltpu.make_async_copy(theirs.at[step], theirs_vmem.at[step], sems.at[2 * step + 1])
        )
    order = list(range(1, outer)) + [0]
    for step in order:
        copies[2 * step].start()
        copies[2 * step + 1].start()
    for step in order:
        copies[2 * step].wait()
        copies[2 * step + 1].wait()
        total = jnp.dot(own_t[...], mine_vmem[step], preferred_element_type=jnp.float32)
        total += jnp.dot(other_t[...], theirs_vmem[step], preferred_element_type=jnp.float32)
        outs[step][...] = total.astype(outs[step].dtype)


def make_local(groups, ways):
    outer = groups // CORES

    def local(
        query_rows, key_rows, value_rows, out_grad, clip_lengths, out_weight, query_gain, key_gain
    ):
        place = lax.axis_index("seq")
        group = lax.axis_index("dp")
        places = jnp.stack([place, group]).astype(jnp.int32)
        rows, features = query_rows.shape[1:]
        width = features // ways
        model = out_grad.shape[2]
        cols = model // groups
        aligned = cols % 128 == 0
        total = ways * rows
        sizes = [h * HEAD_DIM for h in chunk_heads(width // HEAD_DIM)]
        chunks = []
        for size in sizes:
            chunks.append((sum(s for _, s in chunks), size))

        def shift(x, step):
            return lax.ppermute(x, "seq", [(i, (i + step) % ways) for i in range(ways)])

        def partner(x, mask):
            return lax.ppermute(x, "dp", [(i, i ^ mask) for i in range(groups)])

        right, left = [out_grad[0]], [out_grad[0]]
        for step in range(1, ways):
            right.append(
                lax.ppermute(right[-1], "seq", [(i, i + 1) for i in range(step - 1, ways - 1)])
            )
            left.append(
                lax.ppermute(left[-1], "seq", [(i, i - 1) for i in range(1, ways - step + 1)])
            )

        bf16 = jnp.bfloat16
        piece_shapes = [
            jax.ShapeDtypeStruct((3, rows, size), bf16) for _, size in chunks for _ in range(ways)
        ]
        packed = run(
            functools.partial(pack_body, ways=ways, width=width, chunks=chunks),
            piece_shapes,
            (places, query_rows[0], key_rows[0], value_rows[0]),
            [SMEM, ANY, ANY, ANY],
            [ANY] * len(piece_shapes),
            [pltpu.SemaphoreType.DMA((3 * len(piece_shapes),))],
            "pack",
        )
        pieces = []
        for index in range(len(chunks)):
            mine = packed[index * ways : (index + 1) * ways]
            pieces.append([mine[0]] + [shift(mine[step], step) for step in range(1, ways)])

        block = jax.ShapeDtypeStruct((outer, total, cols), bf16)
        extra = [block, block] if aligned else [jax.ShapeDtypeStruct((total, model), bf16)]
        results = run(
            functools.partial(
                d_attn_body,
                ways=ways,
                rows=rows,
                chunks=chunks,
                outer=outer,
                cols=cols,
                aligned=aligned,
            ),
            [jax.ShapeDtypeStruct((total, size), bf16) for _, size in chunks] + extra,
            (places, out_grad[0], *right[1:], *left[1:], out_weight),
            [SMEM] + [ANY] * (2 * ways),
            [VMEM] * len(chunks) + [ANY] * len(extra),
            [
                pltpu.VMEM((total, model), bf16),
                pltpu.VMEM(out_weight.shape, bf16),
                pltpu.SemaphoreType.DMA((ways + 1,)),
                pltpu.SemaphoreType.DMA((2 * outer,)),
            ],
            "d_attn",
        )
        d_attn = results[: len(chunks)]
        if aligned:
            mine, theirs = results[len(chunks) :]
        else:
            full = results[-1]
            core, chip = group % CORES, group // CORES

            def take(step, lane):
                column = ((chip ^ step) * CORES + lane) * cols
                return lax.dynamic_slice_in_dim(full, column, cols, 1)

            mine = jnp.stack([take(step, core) for step in range(outer)])
            theirs = jnp.stack([take(step, 1 - core) for step in range(outer)])
        theirs = partner(theirs, 1)

        gains = 0.0
        back = []
        sums = []
        for index, (start, size) in enumerate(chunks):
            results = run(
                functools.partial(
                    attention_body, ways=ways, rows=rows, heads=size // HEAD_DIM
                ),
                [
                    jax.ShapeDtypeStruct((size, total), bf16),
                    jax.ShapeDtypeStruct((8, HEAD_DIM), jnp.float32),
                ]
                + [jax.ShapeDtypeStruct((3, rows, size), bf16)] * ways,
                (
                    places,
                    clip_lengths,
                    *pieces[index],
                    d_attn[index],
                    query_gain[None],
                    key_gain[None],
                ),
                [SMEM, SMEM] + [VMEM] * (ways + 3),
                [VMEM] * (ways + 2),
                [],
                "attention",
            )
            attn_t, gain_part = results[:2]
            gains = gains + gain_part
            grads = results[2:]
            other_t = partner(attn_t, 1)
            blocks = run(
                functools.partial(weight_body, outer=outer),
                [
                    jax.ShapeDtypeStruct((size, cols), jnp.float32 if step == 0 else bf16)
                    for step in range(outer)
                ],
                (attn_t, other_t, mine, theirs),
                [VMEM, VMEM, ANY, ANY],
                [VMEM] * outer,
                [
                    pltpu.VMEM((outer, total, cols), bf16),
                    pltpu.VMEM((outer, total, cols), bf16),
                    pltpu.SemaphoreType.DMA((2 * outer,)),
                ],
                "weight",
            )
            summed = blocks[0]
            for step in range(1, outer):
                summed = summed + partner(blocks[step], CORES * step).astype(jnp.float32)
            sums.append(summed)
            back.extend([grads[0]] + [shift(grads[step], -step) for step in range(1, ways)])

        outs = run(
            functools.partial(unpack_body, ways=ways, width=width, chunks=chunks),
            [jax.ShapeDtypeStruct((rows, features), bf16)] * 3,
            (places, *back),
            [SMEM] + [ANY] * len(back),
            [ANY] * 3,
            [pltpu.SemaphoreType.DMA((3 * len(back),))],
            "unpack",
        )

        weight_raw = jnp.concatenate(sums, axis=0)
        squares = jnp.sum(weight_raw * weight_raw)
        row = lax.broadcasted_iota(jnp.int32, gains.shape, 0)
        sent = jnp.where(row == 2, squares / HEAD_DIM, gains)
        mask = 1
        while mask < groups:
            sent = sent + partner(sent, mask)
            mask *= 2
        mask = 1
        while mask < ways:
            sent = sent + lax.ppermute(sent, "seq", [(i, i ^ mask) for i in range(ways)])
            mask *= 2
        qgain_raw, kgain_raw = sent[0], sent[1]
        grad_norm = jnp.sqrt(
            jnp.sum(sent[2]) + jnp.sum(qgain_raw * qgain_raw) + jnp.sum(kgain_raw * kgain_raw)
        )
        factor = jnp.minimum(jnp.float32(1.0), MAX_NORM / (grad_norm + EPS))
        return (
            outs[0][None],
            outs[1][None],
            outs[2][None],
            weight_raw * factor,
            qgain_raw * factor,
            kgain_raw * factor,
            grad_norm,
        )

    return local


def solution(mesh):
    rows = P("dp", "seq", None)
    return jax.shard_map(
        make_local(mesh.shape["dp"], mesh.shape["seq"]),
        mesh=mesh,
        in_specs=(rows, rows, rows, rows, P("dp", None), P("seq", None), P(), P()),
        out_specs=(rows, rows, rows, P("seq", "dp"), P(), P(), P()),
        check_vma=False,
    )
```

```python
import functools
import jax
import jax.numpy as jnp
from jax import lax
from jax.experimental import pallas as pl
from jax.experimental.pallas import tpu as pltpu
from jax.sharding import PartitionSpec as P

HEAD_DIM = 128
MAX_NORM = 768
EPS = 1e-06
CORES = 2
CHUNKS = 3
HALVES = 2
LOADS = 1
TOGETHER = 3
VMEM_BYTES = 40 * 1024 * 1024


ANY = pl.BlockSpec(memory_space=pl.ANY)
SMEM = pl.BlockSpec(memory_space=pltpu.SMEM)
VMEM = pl.BlockSpec(memory_space=pltpu.VMEM)


def run(body, outs, args, in_specs, out_specs, scratch=(), grid=None):
    return pl.pallas_call(
        body,
        out_shape=outs,
        grid=() if grid is None else grid,
        in_specs=in_specs,
        out_specs=out_specs,
        scratch_shapes=list(scratch),
        compiler_params=pltpu.CompilerParams(vmem_limit_bytes=VMEM_BYTES),
    )(*args)


def chunk_count(heads):
    return max(c for c in range(1, CHUNKS + 1) if heads % c == 0)


def dot(a, b, dims=(1, 0)):
    contract = (((dims[0],), (dims[1],)), ((), ()))
    return lax.dot_general(a, b, contract, preferred_element_type=jnp.float32)


def pack_body(place_ref, *refs, ways, width):
    rows, outs = refs[:3], refs[3:]
    place = place_ref[0]
    for step in range(ways):
        column = pl.multiple_of(lax.rem(place + step, ways) * width, 128)
        for which in range(3):
            outs[step][which] = rows[which][:, pl.ds(column, width)]


def unpack_body(place_ref, *refs, ways, width, size):
    pieces, outs = refs[:-3], refs[-3:]
    place = place_ref[0]
    for slot, piece in enumerate(pieces):
        start, step = slot // ways * size, slot % ways
        column = pl.multiple_of(lax.rem(place + step, ways) * width + start, 128)
        for which in range(3):
            outs[which][:, pl.ds(column, size)] = piece[which]


def item_of(place, index, ways):
    both = jnp.minimum(place, ways - 1 - place)
    paired = index <= 2 * both
    hops = jnp.where(paired, (index + 1) // 2, index - both)
    lefty = jnp.where(paired, index % 2 == 1, 2 * place > ways - 1)
    return hops, lefty


def slot_of(place, index, ways):
    if index == 0:
        return jnp.int32(0)
    hops, lefty = item_of(place, index, ways)
    return jnp.where(lefty, hops, ways - hops)


def d_attn_body(place_ref, *refs, index, ways, groups, hops_list, rows, cols, aligned):
    pieces = HALVES if index == 0 else 2 * HALVES * len(hops_list)
    sources = refs[:pieces]
    weight = refs[pieces]
    outs = refs[pieces + 1 : -4]
    full, weight_vmem, sems, out_sems = refs[-4:]
    place = place_ref[0]
    group = place_ref[1]
    part = rows // HALVES
    depth = weight.shape[1] // LOADS
    loads = []
    for i in range(LOADS):
        at = pl.ds(i * depth, depth)
        loads.append(
            pltpu.make_async_copy(
                weight.at[:, at], weight_vmem.at[:, at], sems.at[HALVES + i]
            )
        )

    def fetch(first):
        return [
            pltpu.make_async_copy(
                sources[first + half], full.at[pl.ds(half * part, part)], sems.at[half]
            )
            for half in range(HALVES)
        ]

    def begin(first):
        for copy in fetch(first):
            copy.start()

    if index == 0:
        begin(0)
    else:
        hops, lefty = item_of(place, index, ways)
        for i, dist in enumerate(hops_list):
            for side in range(2):
                here = jnp.logical_and(hops == dist, lefty == (side == 0))

                @pl.when(here)
                def _(first=(2 * i + side) * HALVES):
                    begin(first)

    for load in loads:
        load.start()
    for copy in fetch(0):
        copy.wait()
    writes = []
    if aligned:
        for mask in range(groups):
            column = pl.multiple_of(lax.bitwise_xor(group, mask) * cols, 128)
            writes.append(
                pltpu.make_async_copy(
                    full.at[:, pl.ds(column, cols)], outs[1 + mask], out_sems.at[mask]
                )
            )
    else:
        writes.append(pltpu.make_async_copy(full, outs[1], out_sems.at[0]))
    for write in writes:
        write.start()
    total = None
    for i, load in enumerate(loads):
        load.wait()
        at = slice(i * depth, (i + 1) * depth)
        term = dot(full[:, at], weight_vmem[:, at], (1, 1))
        total = term if total is None else total + term
    outs[0][...] = total.astype(jnp.bfloat16)
    for write in writes:
        write.wait()


def segments(place, lengths_ref, shape, dim, ways, rows):
    index = lax.broadcasted_iota(jnp.int32, shape, dim)
    source = place - lax.div(index, rows)
    source = jnp.where(source < 0, source + ways, source)
    position = source * rows + lax.rem(index, rows)
    seg = jnp.zeros(shape, jnp.int32)
    end = jnp.int32(0)
    for clip in range(lengths_ref.shape[1]):
        end = end + lengths_ref[0, clip]
        seg = seg + (position >= end).astype(jnp.int32)
    return seg


def norm_rows(raw, gain):
    wide = raw.astype(jnp.float32)
    inverse = lax.rsqrt(jnp.mean(wide * wide, axis=-1, keepdims=True) + EPS)
    unit = wide * inverse
    return unit, inverse, (unit * gain).astype(jnp.bfloat16)


def norm_back(unit, inverse, gain, d_norm):
    d_unit = d_norm * gain
    grad = inverse * (d_unit - unit * jnp.mean(unit * d_unit, axis=-1, keepdims=True))
    return grad.astype(jnp.bfloat16), jnp.sum(unit * d_norm, axis=0, keepdims=True)


def forward_body(place_ref, lengths_ref, *refs, ways, rows):
    pieces = refs[:ways]
    q_gain_ref, k_gain_ref, attn_t_ref, probs_ref = refs[ways:]
    total = ways * rows
    place = place_ref[0]
    scale = HEAD_DIM ** (-0.5)
    same = segments(place, lengths_ref, (total, 1), 0, ways, rows) == segments(
        place, lengths_ref, (1, total), 1, ways, rows
    )

    def gather(which):
        return jnp.concatenate([piece[which] for piece in pieces], axis=0)

    _, _, q_norm = norm_rows(gather(0), q_gain_ref[...])
    _, _, k_norm = norm_rows(gather(1), k_gain_ref[...])
    value = gather(2)
    scores = dot(k_norm, q_norm, (1, 1)) * scale
    expo = jnp.where(same, jnp.exp(scores), 0.0)
    inverse_sum = 1.0 / jnp.sum(expo, axis=0, keepdims=True)
    probs = (expo * inverse_sum).astype(jnp.bfloat16)
    probs_ref[0] = probs
    attn_t_ref[...] = dot(value.T, probs).astype(jnp.bfloat16)


def backward_body(place_ref, *refs, ways, rows, heads):
    pieces = refs[:ways]
    d_pieces = refs[ways : 2 * ways]
    probs_ref, q_gain_ref, k_gain_ref, gains_ref = refs[2 * ways : 2 * ways + 4]
    outs = refs[2 * ways + 4 : 3 * ways + 4]
    d_attn_ref = refs[-1]
    place = place_ref[0]
    scale = HEAD_DIM ** (-0.5)
    for index in range(ways):
        row = pl.multiple_of(slot_of(place, index, ways) * rows, rows)
        d_attn_ref[pl.ds(row, rows), :] = d_pieces[index][...]
    q_gain = q_gain_ref[...]
    k_gain = k_gain_ref[...]
    q_sum = jnp.zeros((1, HEAD_DIM), jnp.float32)
    k_sum = jnp.zeros((1, HEAD_DIM), jnp.float32)
    for head in range(heads):
        part = slice(head * HEAD_DIM, (head + 1) * HEAD_DIM)

        def gather(which):
            return jnp.concatenate([piece[which, :, part] for piece in pieces], axis=0)

        q_unit, q_inv, q_norm = norm_rows(gather(0), q_gain)
        k_unit, k_inv, k_norm = norm_rows(gather(1), k_gain)
        value = gather(2)
        d_attn = d_attn_ref[:, part]
        probs = probs_ref[head]
        d_probs = dot(value, d_attn, (1, 1))
        probs32 = probs.astype(jnp.float32)
        row_sum = jnp.sum(probs32 * d_probs, axis=0, keepdims=True)
        d_scores = (probs32 * (d_probs - row_sum) * scale).astype(jnp.bfloat16)
        d_value = dot(probs, d_attn).astype(jnp.bfloat16)
        d_k = dot(d_scores, q_norm)
        d_q = dot(k_norm.T, d_scores).T
        q_grad, q_part = norm_back(q_unit, q_inv, q_gain, d_q)
        k_grad, k_part = norm_back(k_unit, k_inv, k_gain, d_k)
        q_sum = q_sum + q_part
        k_sum = k_sum + k_part
        for step in range(ways):
            block = slice(step * rows, (step + 1) * rows)
            outs[step][0, :, part] = q_grad[block]
            outs[step][1, :, part] = k_grad[block]
            outs[step][2, :, part] = d_value[block]
    gains_ref[...] = jnp.concatenate(
        [q_sum, k_sum, jnp.zeros((6, HEAD_DIM), jnp.float32)], axis=0
    )


def weight_body(place_ref, *refs, items, ways, groups, rows, first, last):
    attn = refs[:groups]
    columns = refs[groups : (1 + len(items)) * groups]
    out = refs[(1 + len(items)) * groups + (0 if first else 1)]
    left, right, before, sems, before_sem = refs[-5:]
    if not first:
        fetch = pltpu.make_async_copy(refs[(1 + len(items)) * groups], before, before_sem)
        fetch.start()
    copies = []
    for i, index in enumerate(items):
        slot = pl.multiple_of(slot_of(place_ref[0], index, ways) * rows, 128)
        copies.append([])
        for mask in range(groups):
            at = pl.ds(mask * rows, rows)
            source = attn[mask].at[:, pl.ds(slot, rows)]
            copies[-1].append(
                pltpu.make_async_copy(source, left.at[i, :, at], sems.at[i, 2 * mask])
            )
            source = columns[i * groups + mask]
            copies[-1].append(
                pltpu.make_async_copy(source, right.at[i, at], sems.at[i, 2 * mask + 1])
            )
    for group in copies:
        for copy in group:
            copy.start()
    total = None
    for i, group in enumerate(copies):
        for copy in group:
            copy.wait()
        term = dot(left[i], right[i])
        total = term if total is None else total + term
    if not first:
        fetch.wait()
        total = total + before[...]
    out[...] = total
    if last:
        refs[(1 + len(items)) * groups + 2][...] = jnp.sum(total * total, axis=0, keepdims=True)


def weight_items(ways):
    count = ways - 1
    starts = range(0, count, TOGETHER)
    return [list(range(i, min(i + TOGETHER, count))) for i in starts] + [[count]]


def make_local(groups, ways):
    def local(
        query_rows, key_rows, value_rows, out_grad, clip_lengths, out_weight, query_gain, key_gain
    ):
        place = lax.axis_index("seq")
        group = lax.axis_index("dp")
        places = jnp.stack([place, group]).astype(jnp.int32)
        rows, features = query_rows.shape[1:]
        width = features // ways
        heads = width // HEAD_DIM
        count = chunk_count(heads)
        size = width // count
        model = out_grad.shape[2]
        cols = model // groups
        aligned = cols % 128 == 0
        total = ways * rows
        bf16 = jnp.bfloat16
        f32 = jnp.float32
        barrier = lax.optimization_barrier

        def struct(*shape, dtype=bf16):
            return jax.ShapeDtypeStruct(shape, dtype)

        def shift(x, step):
            return lax.ppermute(x, "seq", [(i, (i + step) % ways) for i in range(ways)])

        def partner(x, mask):
            return lax.ppermute(x, "dp", [(i, i ^ mask) for i in range(groups)])

        packed = run(
            functools.partial(pack_body, ways=ways, width=width),
            [struct(3, rows, width)] * ways,
            (places, query_rows[0], key_rows[0], value_rows[0]),
            [SMEM, VMEM, VMEM, VMEM],
            [VMEM] * ways,
        )
        pieces = [packed[0]] + [shift(packed[step], step) for step in range(1, ways)]

        extra = [struct(rows, cols)] * groups if aligned else [struct(rows, model)]
        part = rows // HALVES
        own = [out_grad[0, half * part : (half + 1) * part] for half in range(HALVES)]
        right, left = [own], [own]
        d_attn, columns = [], []
        for index in range(ways):
            if index > 0:
                up = [(i, i + 1) for i in range(index - 1, ways - 1)]
                down = [(i, i - 1) for i in range(1, ways - index + 1)]
                right.append([])
                left.append([])
                for half in range(HALVES):
                    right[-1].append(lax.ppermute(right[-2][half], "seq", up))
                    left[-1].append(lax.ppermute(left[-2][half], "seq", down))
            hops_list = list(range((index + 1) // 2, index + 1)) if index else []
            sources = [x for dist in hops_list for side in (right, left) for x in side[dist]] or own
            results = run(
                functools.partial(
                    d_attn_body,
                    index=index,
                    ways=ways,
                    groups=groups,
                    hops_list=hops_list,
                    rows=rows,
                    cols=cols,
                    aligned=aligned,
                ),
                [struct(rows, width)] + extra,
                (places, *sources, out_weight),
                [SMEM] + [ANY] * (len(sources) + 1),
                [VMEM] + [ANY] * len(extra),
                [
                    pltpu.VMEM((rows, model), bf16),
                    pltpu.VMEM(out_weight.shape, bf16),
                    pltpu.SemaphoreType.DMA((HALVES + LOADS,)),
                    pltpu.SemaphoreType.DMA((groups,)),
                ],
            )
            d_attn.append(results[0])
            blocks = results[1:]
            if not aligned:
                blocks = [
                    lax.dynamic_slice_in_dim(results[1], (group ^ mask) * cols, cols, 1)
                    for mask in range(groups)
                ]
            got = {mask: partner(blocks[mask], mask) for mask in reversed(range(1, groups))}
            columns.append([blocks[0]] + [got[mask] for mask in range(1, groups)])

        attn_t, probs = run(
            functools.partial(forward_body, ways=ways, rows=rows),
            [struct(width, total), struct(heads, total, total)],
            (places, clip_lengths, *pieces, query_gain[None], key_gain[None]),
            [SMEM, SMEM]
            + [pl.BlockSpec((3, rows, HEAD_DIM), lambda h: (0, 0, h))] * ways
            + [pl.BlockSpec((1, HEAD_DIM), lambda h: (0, 0))] * 2,
            [
                pl.BlockSpec((HEAD_DIM, total), lambda h: (h, 0)),
                pl.BlockSpec((1, total, total), lambda h: (h, 0, 0)),
            ],
            grid=(heads,),
        )
        attn = [attn_t]
        for mask in range(1, groups):
            if mask % CORES:
                attn.append(partner(attn[mask - 1], 1))
            else:
                attn.append(partner(attn_t, mask))

        gains = 0.0
        back = []
        for index in range(count):
            results = run(
                functools.partial(
                    backward_body, ways=ways, rows=rows, heads=size // HEAD_DIM
                ),
                [struct(8, HEAD_DIM, dtype=f32)] + [struct(3, rows, size)] * ways,
                (places, *pieces, *d_attn, probs, query_gain[None], key_gain[None]),
                [SMEM]
                + [pl.BlockSpec((3, rows, size), lambda i, at=index: (0, 0, at))] * ways
                + [pl.BlockSpec((rows, size), lambda i, at=index: (0, at))] * ways
                + [pl.BlockSpec((size // HEAD_DIM, total, total), lambda i, at=index: (at, 0, 0))]
                + [pl.BlockSpec((1, HEAD_DIM), lambda i: (0, 0))] * 2,
                [pl.BlockSpec((8, HEAD_DIM), lambda i: (0, 0))]
                + [pl.BlockSpec((3, rows, size), lambda i: (0, 0, 0))] * ways,
                [pltpu.VMEM((total, size), bf16)],
                grid=(1,),
            )
            gains = gains + results[0]
            grads = results[1:]
            back.extend([grads[0]] + [shift(grads[step], -step) for step in range(1, ways)])

        weight_raw = None
        for items in weight_items(ways):
            first, last = weight_raw is None, items[-1] == ways - 1
            results = run(
                functools.partial(
                    weight_body,
                    items=items,
                    ways=ways,
                    groups=groups,
                    rows=rows,
                    first=first,
                    last=last,
                ),
                [struct(width, cols, dtype=f32)]
                + ([struct(1, cols, dtype=f32)] if last else []),
                (places, *attn)
                + tuple(x for index in items for x in columns[index])
                + (() if first else (weight_raw,)),
                [SMEM] + [ANY] * ((1 + len(items)) * groups + (0 if first else 1)),
                [VMEM] * (2 if last else 1),
                [
                    pltpu.VMEM((len(items), width, groups * rows), bf16),
                    pltpu.VMEM((len(items), groups * rows, cols), bf16),
                    pltpu.VMEM((width, cols), f32),
                    pltpu.SemaphoreType.DMA((len(items), 2 * groups)),
                    pltpu.SemaphoreType.DMA,
                ],
            )
            weight_raw = results[0]

        squares = jnp.sum(results[1])
        row = lax.broadcasted_iota(jnp.int32, gains.shape, 0)
        sent = jnp.where(row == 2, squares / HEAD_DIM, gains)
        mask = 1
        while mask < groups:
            sent = sent + partner(sent, mask)
            mask *= 2
        mask = 1
        while mask < ways:
            sent = sent + lax.ppermute(sent, "seq", [(i, i ^ mask) for i in range(ways)])
            mask *= 2
        qgain_raw, kgain_raw = sent[0], sent[1]
        grad_norm = jnp.sqrt(
            jnp.sum(sent[2]) + jnp.sum(qgain_raw * qgain_raw) + jnp.sum(kgain_raw * kgain_raw)
        )
        factor = jnp.minimum(jnp.float32(1.0), MAX_NORM / (grad_norm + EPS))
        weight_grad = weight_raw * factor
        tail = back[-ways + 1 :]
        tail, weight_grad = barrier((tail, weight_grad))
        back = back[: -ways + 1] + tail
        outs = run(
            functools.partial(unpack_body, ways=ways, width=width, size=size),
            [struct(rows, features)] * 3,
            (places, *back),
            [SMEM] + [VMEM] * len(back),
            [VMEM] * 3,
        )

        return (
            outs[0][None],
            outs[1][None],
            outs[2][None],
            weight_grad,
            qgain_raw * factor,
            kgain_raw * factor,
            grad_norm,
        )

    return local


def solution(mesh):
    rows = P("dp", "seq", None)
    groups, ways = mesh.shape["dp"], mesh.shape["seq"]
    body = make_local(groups, ways)

    return jax.shard_map(
        body,
        mesh=mesh,
        in_specs=(rows, rows, rows, rows, P("dp", None), P("seq", None), P(), P()),
        out_specs=(rows, rows, rows, P("seq", "dp"), P(), P(), P()),
        check_vma=False,
    )
```

```python
import functools
import math
import jax
import jax.numpy as jnp
from jax import lax
from jax.experimental import pallas as pl
from jax.experimental.pallas import tpu as pltpu
from jax.sharding import PartitionSpec as P

HEAD_DIM = 128
MAX_NORM = 768
EPS = 1e-06
CORES = 2
CHUNKS = 3
HALVES = 2
TOGETHER = 3
MIB = 1024 * 1024


ANY = pl.BlockSpec(memory_space=pl.ANY)
SMEM = pl.BlockSpec(memory_space=pltpu.SMEM)
VMEM = pl.BlockSpec(memory_space=pltpu.VMEM)


def run(body, outs, args, in_specs, out_specs, scratch=(), grid=None, room=0, alias=None):
    return pl.pallas_call(
        body,
        out_shape=outs,
        grid=() if grid is None else grid,
        in_specs=in_specs,
        out_specs=out_specs,
        scratch_shapes=list(scratch),
        input_output_aliases=alias or {},
        compiler_params=pltpu.CompilerParams(vmem_limit_bytes=min(room + 4 * MIB, 62 * MIB)),
    )(*args)


def size_of(*arrays):
    return sum(math.prod(x.shape) * x.dtype.itemsize for x in arrays)


def chunk_count(heads):
    return max(c for c in range(1, CHUNKS + 1) if heads % c == 0)


def dot(a, b, dims=(1, 0)):
    contract = (((dims[0],), (dims[1],)), ((), ()))
    return lax.dot_general(a, b, contract, preferred_element_type=jnp.float32)


def pack_body(place_ref, *refs, ways, width):
    rows, outs = refs[:3], refs[3:]
    place = place_ref[0]
    for step in range(ways):
        column = pl.multiple_of(lax.rem(place + step, ways) * width, 128)
        for which in range(3):
            outs[step][which] = rows[which][:, pl.ds(column, width)]


def unpack_body(place_ref, *refs, ways, width, start, size, finish):
    pieces, sems = refs[:ways], refs[-1]
    outs = refs[-8:-5] if finish else refs[-4:-1]
    copies = []
    for step, piece in enumerate(pieces):
        column = pl.multiple_of(lax.rem(place_ref[0] + step, ways) * width + start, 128)
        for which in range(3):
            target = outs[which].at[:, pl.ds(column, size)]
            copies.append(pltpu.make_async_copy(piece.at[which], target, sems.at[step, which]))
    for copy in copies:
        copy.start()
    if finish:
        grad_ref, q_ref, k_ref, norm_ref = refs[-5:-1]
        weight_ref, parts = refs[ways], refs[ways + 1 : ways + 1 + finish]
        total = sum(part[...] for part in parts)
        q_gain, k_gain = total[0:1], total[1:2]
        squares = total[2:3] + q_gain * q_gain + k_gain * k_gain
        norm = jnp.sqrt(jnp.sum(squares, axis=1, keepdims=True))
        factor = jnp.minimum(jnp.float32(1.0), MAX_NORM / (norm + EPS))
        grad_ref[...] = weight_ref[...] * factor
        q_ref[...] = q_gain * factor
        k_ref[...] = k_gain * factor
        norm_ref[...] = norm
    for copy in copies:
        copy.wait()


def item_of(place, index, ways):
    both = jnp.minimum(place, ways - 1 - place)
    paired = index <= 2 * both
    hops = jnp.where(paired, (index + 1) // 2, index - both)
    lefty = jnp.where(paired, index % 2 == 1, 2 * place > ways - 1)
    return hops, lefty


def slot_of(place, index, ways):
    if index == 0:
        return jnp.int32(0)
    hops, lefty = item_of(place, index, ways)
    return jnp.where(lefty, hops, ways - hops)


def d_attn_body(place_ref, *refs, index, ways, groups, hops_list, parts, rows, cols, aligned, span, emit):
    count = sum(parts) * (2 if index else 1)
    sources, weight = refs[:count], refs[count]
    outs, full = refs[count + 1 : -1], refs[-1]
    place, group = place_ref[0], place_ref[1]

    def take(pieces):
        height = rows // len(pieces)
        for i, piece in enumerate(pieces):
            full[i * height : (i + 1) * height, :] = piece[...]

    if index == 0:
        take(sources)
    else:
        hops, lefty = item_of(place, index, ways)
        at = 0
        for dist, number in zip(hops_list, parts):
            for side in range(2):
                here = jnp.logical_and(hops == dist, lefty == (side == 0))
                pl.when(here)(functools.partial(take, sources[at : at + number]))
                at += number

    part = weight[span[0] : span[1], :]
    outs[0][...] = dot(full[...], part, (1, 1)).astype(jnp.bfloat16)
    if not emit:
        return
    if aligned:
        for mask in range(groups):
            column = pl.multiple_of(lax.bitwise_xor(group, mask) * cols, 128)
            outs[1 + mask][...] = full[:, pl.ds(column, cols)]
    else:
        outs[1][...] = full[...]


def segments(place, lengths_ref, shape, dim, ways, rows):
    index = lax.broadcasted_iota(jnp.int32, shape, dim)
    source = place - lax.div(index, rows)
    source = jnp.where(source < 0, source + ways, source)
    position = source * rows + lax.rem(index, rows)
    seg = jnp.zeros(shape, jnp.int32)
    end = jnp.int32(0)
    for clip in range(lengths_ref.shape[1]):
        end = end + lengths_ref[0, clip]
        seg = seg + (position >= end).astype(jnp.int32)
    return seg


def norm_rows(raw, gain):
    wide = raw.astype(jnp.float32)
    inverse = lax.rsqrt(jnp.mean(wide * wide, axis=-1, keepdims=True) + EPS)
    unit = wide * inverse
    return unit, inverse, (unit * gain).astype(jnp.bfloat16)


def norm_back(unit, inverse, gain, d_norm):
    d_unit = d_norm * gain
    grad = inverse * (d_unit - unit * jnp.mean(unit * d_unit, axis=-1, keepdims=True))
    return grad.astype(jnp.bfloat16), jnp.sum(unit * d_norm, axis=0, keepdims=True)


def forward_body(place_ref, lengths_ref, *refs, ways, rows):
    pieces = refs[:ways]
    q_gain_ref, k_gain_ref, attn_t_ref, probs_ref = refs[ways:]
    total = ways * rows
    place = place_ref[0]
    scale = HEAD_DIM ** (-0.5)
    same = segments(place, lengths_ref, (total, 1), 0, ways, rows) == segments(
        place, lengths_ref, (1, total), 1, ways, rows
    )

    def gather(which):
        return jnp.concatenate([piece[which] for piece in pieces], axis=0)

    _, _, q_norm = norm_rows(gather(0), q_gain_ref[...])
    _, _, k_norm = norm_rows(gather(1), k_gain_ref[...])
    value = gather(2)
    scores = dot(k_norm, q_norm, (1, 1)) * scale
    expo = jnp.where(same, jnp.exp(scores), 0.0)
    inverse_sum = 1.0 / jnp.sum(expo, axis=0, keepdims=True)
    probs = (expo * inverse_sum).astype(jnp.bfloat16)
    probs_ref[0] = probs
    attn_t_ref[...] = dot(value.T, probs).astype(jnp.bfloat16)


def backward_body(place_ref, *refs, ways, rows, heads):
    pieces = refs[:ways]
    d_pieces = refs[ways : 2 * ways]
    probs_ref, q_gain_ref, k_gain_ref, gains_ref = refs[2 * ways : 2 * ways + 4]
    outs = refs[2 * ways + 4 : 3 * ways + 4]
    d_attn_ref = refs[-1]
    place = place_ref[0]
    scale = HEAD_DIM ** (-0.5)
    for index in range(ways):
        row = pl.multiple_of(slot_of(place, index, ways) * rows, rows)
        d_attn_ref[pl.ds(row, rows), :] = d_pieces[index][...]
    q_gain = q_gain_ref[...]
    k_gain = k_gain_ref[...]
    q_sum = jnp.zeros((1, HEAD_DIM), jnp.float32)
    k_sum = jnp.zeros((1, HEAD_DIM), jnp.float32)
    for head in range(heads):
        part = slice(head * HEAD_DIM, (head + 1) * HEAD_DIM)

        def gather(which):
            return jnp.concatenate([piece[which, :, part] for piece in pieces], axis=0)

        q_unit, q_inv, q_norm = norm_rows(gather(0), q_gain)
        k_unit, k_inv, k_norm = norm_rows(gather(1), k_gain)
        value = gather(2)
        d_attn = d_attn_ref[:, part]
        probs = probs_ref[head]
        d_probs = dot(value, d_attn, (1, 1))
        probs32 = probs.astype(jnp.float32)
        row_sum = jnp.sum(probs32 * d_probs, axis=0, keepdims=True)
        d_scores = (probs32 * (d_probs - row_sum) * scale).astype(jnp.bfloat16)
        d_value = dot(probs, d_attn).astype(jnp.bfloat16)
        d_k = dot(d_scores, q_norm)
        d_q = dot(k_norm.T, d_scores).T
        q_grad, q_part = norm_back(q_unit, q_inv, q_gain, d_q)
        k_grad, k_part = norm_back(k_unit, k_inv, k_gain, d_k)
        q_sum = q_sum + q_part
        k_sum = k_sum + k_part
        for step in range(ways):
            block = slice(step * rows, (step + 1) * rows)
            outs[step][0, :, part] = q_grad[block]
            outs[step][1, :, part] = k_grad[block]
            outs[step][2, :, part] = d_value[block]
    gains_ref[...] = jnp.concatenate(
        [q_sum, k_sum, jnp.zeros((6, HEAD_DIM), jnp.float32)], axis=0
    )


def weight_body(place_ref, *refs, items, ways, groups, rows, first, last):
    attn = refs[:groups]
    columns = refs[groups : (1 + len(items)) * groups]
    outs = refs[-2:] if last else refs[-1:]
    gain_refs = refs[(1 + len(items)) * groups + 1 : -2]
    left = []
    for index in items:
        slot = pl.multiple_of(slot_of(place_ref[0], index, ways) * rows, 128)
        left += [piece[:, pl.ds(slot, rows)] for piece in attn]
    right = [piece[...] for piece in columns]
    total = dot(jnp.concatenate(left, axis=1), jnp.concatenate(right, axis=0))
    if not first:
        total = total + refs[(1 + len(items)) * groups][...]
    outs[0][...] = total
    if last:
        squares = jnp.sum(jnp.sum(total * total, axis=0, keepdims=True), axis=1, keepdims=True)
        gains = sum(ref[...] for ref in gain_refs)
        row = lax.broadcasted_iota(jnp.int32, gains.shape, 0)
        outs[1][...] = gains + jnp.where(row == 2, squares / HEAD_DIM, 0.0)


def weight_items(ways):
    count = ways - 1
    starts = range(0, count, TOGETHER)
    return [list(range(i, min(i + TOGETHER, count))) for i in starts] + [[count]]


def make_local(groups, ways):
    def local(
        query_rows, key_rows, value_rows, out_grad, clip_lengths, out_weight, query_gain, key_gain
    ):
        place = lax.axis_index("seq")
        group = lax.axis_index("dp")
        places = jnp.stack([place, group]).astype(jnp.int32)
        rows, features = query_rows.shape[1:]
        width = features // ways
        heads = width // HEAD_DIM
        count = chunk_count(heads)
        size = width // count
        model = out_grad.shape[2]
        cols = model // groups
        aligned = cols % 128 == 0
        total = ways * rows
        bf16 = jnp.bfloat16
        f32 = jnp.float32
        lanes = -(-cols // 128) * 128

        def struct(*shape, dtype=bf16):
            return jax.ShapeDtypeStruct(shape, dtype)

        def shift(x, step):
            return lax.ppermute(x, "seq", [(i, (i + step) % ways) for i in range(ways)])

        def partner(x, mask):
            return lax.ppermute(x, "dp", [(i, i ^ mask) for i in range(groups)])

        packed = run(
            functools.partial(pack_body, ways=ways, width=width),
            [struct(3, rows, width)] * ways,
            (places, query_rows[0], key_rows[0], value_rows[0]),
            [SMEM, VMEM, VMEM, VMEM],
            [VMEM] * ways,
            room=6 * size_of(query_rows),
        )
        pieces = [packed[0]] + [shift(packed[step], step) for step in range(1, ways)]

        extra = [struct(rows, cols)] * groups if aligned else [struct(rows, model)]
        right, left = [[out_grad[0]]], [[out_grad[0]]]
        d_attn, columns = [], []
        for index in range(ways):
            if index > 0:
                up = [(i, i + 1) for i in range(index - 1, ways - 1)]
                down = [(i, i - 1) for i in range(1, ways - index + 1)]
                if index == 2:
                    part = rows // HALVES
                    sent = [
                        [side[1][0][half * part : (half + 1) * part] for half in range(HALVES)]
                        for side in (right, left)
                    ]
                else:
                    sent = [right[-1], left[-1]]
                right.append([])
                left.append([])
                for half in range(len(sent[0])):
                    right[-1].append(lax.ppermute(sent[0][half], "seq", up))
                    left[-1].append(lax.ppermute(sent[1][half], "seq", down))
            hops_list = list(range((index + 1) // 2, index + 1)) if index else [0]
            sources = [x for dist in hops_list for side in (right, left) for x in side[dist]]
            if index == 0:
                sources = [out_grad[0]]

            def piece(span, emit):
                return run(
                    functools.partial(
                        d_attn_body,
                        index=index,
                        ways=ways,
                        groups=groups,
                        hops_list=hops_list,
                        parts=[len(right[dist]) for dist in hops_list],
                        rows=rows,
                        cols=cols,
                        aligned=aligned,
                        span=span,
                        emit=emit,
                    ),
                    [struct(rows, span[1] - span[0])] + (extra if emit else []),
                    (places, *sources, out_weight),
                    [SMEM] + [VMEM] * (len(sources) + 1),
                    [VMEM] * (1 + (len(extra) if emit else 0)),
                    [pltpu.VMEM((rows, model), bf16)],
                    room=size_of(out_weight, out_grad, out_grad, *sources),
                )

            lead = []
            if index == ways - 1 and count > 1:
                lead = piece((0, size), False)
            results = piece((size if lead else 0, width), True)
            d_attn.append((*lead, results[0]))
            blocks = results[1:]
            if not aligned:
                blocks = [
                    lax.dynamic_slice_in_dim(results[1], (group ^ mask) * cols, cols, 1)
                    for mask in range(groups)
                ]
            got = {mask: partner(blocks[mask], mask) for mask in reversed(range(1, groups))}
            columns.append([blocks[0]] + [got[mask] for mask in range(1, groups)])

        attn_t, probs = run(
            functools.partial(forward_body, ways=ways, rows=rows),
            [struct(width, total), struct(heads, total, total)],
            (places, clip_lengths, *pieces, query_gain[None], key_gain[None]),
            [SMEM, SMEM]
            + [pl.BlockSpec((3, rows, HEAD_DIM), lambda h: (0, 0, h))] * ways
            + [pl.BlockSpec((1, HEAD_DIM), lambda h: (0, 0))] * 2,
            [
                pl.BlockSpec((HEAD_DIM, total), lambda h: (h, 0)),
                pl.BlockSpec((1, total, total), lambda h: (h, 0, 0)),
            ],
            grid=(heads,),
            room=24 * total * total + 4 * MIB,
        )
        attn = [attn_t]
        for mask in range(1, groups):
            if mask % CORES:
                attn.append(partner(attn[mask - 1], 1))
            else:
                attn.append(partner(attn_t, mask))

        gains = []
        back = []
        for index in range(count):
            results = run(
                functools.partial(
                    backward_body, ways=ways, rows=rows, heads=size // HEAD_DIM
                ),
                [struct(8, HEAD_DIM, dtype=f32)] + [struct(3, rows, size)] * ways,
                (places, *pieces, *[x[-1 if index else 0] for x in d_attn], probs, query_gain[None], key_gain[None]),
                [SMEM]
                + [pl.BlockSpec((3, rows, size), lambda i, at=index: (0, 0, at))] * ways
                + [
                    pl.BlockSpec((rows, size), lambda i, at=max(0, index + 1 - len(x)): (0, at))
                    for x in d_attn
                ]
                + [pl.BlockSpec((size // HEAD_DIM, total, total), lambda i, at=index: (at, 0, 0))]
                + [pl.BlockSpec((1, HEAD_DIM), lambda i: (0, 0))] * 2,
                [pl.BlockSpec((8, HEAD_DIM), lambda i: (0, 0))]
                + [pl.BlockSpec((3, rows, size), lambda i: (0, 0, 0))] * ways,
                [pltpu.VMEM((total, size), bf16)],
                grid=(1,),
                room=(20 + 4 * (size // HEAD_DIM)) * total * total + 4 * MIB,
            )
            gains.append(results[0])
            grads = results[1:]
            back.append(grads[0])
            for step in range(1, ways):
                back.append(shift(grads[step], -step))

        weight_raw = None
        for items in weight_items(ways):
            first, last = weight_raw is None, items[-1] == ways - 1
            results = run(
                functools.partial(
                    weight_body,
                    items=items,
                    ways=ways,
                    groups=groups,
                    rows=rows,
                    first=first,
                    last=last,
                ),
                [struct(width, cols, dtype=f32)]
                + ([struct(8, HEAD_DIM, dtype=f32)] if last else []),
                (places, *attn)
                + tuple(x for index in items for x in columns[index])
                + (() if first else (weight_raw,))
                + (tuple(gains) if last else ()),
                [SMEM]
                + [VMEM]
                * ((1 + len(items)) * groups + (0 if first else 1) + (len(gains) if last else 0)),
                [VMEM] * (2 if last else 1),
                room=groups * (total * width + len(items) * rows * (lanes + width)) * 2
                + 12 * width * lanes,
            )
            weight_raw = results[0]

        parts = [results[1]]
        for axis, number in (("dp", groups), ("seq", ways)):
            mask = 1
            while mask < number:
                radix = 4 if mask * 4 <= number and (axis == "seq" or mask > 1) else 2
                sent = sum(parts[1:], parts[0])
                parts = [sent]
                for step in range(1, radix):
                    if axis == "dp":
                        parts.append(partner(sent, mask * step))
                    else:
                        aside = 0
                        pairs = [
                            (d * ways + i, (d ^ aside) * ways + (i ^ (mask * step)))
                            for d in range(groups)
                            for i in range(ways)
                        ]
                        parts.append(lax.ppermute(sent, ("dp", "seq"), pairs))
                mask *= radix
        outs = ()
        for index in range(count):
            last = index == count - 1
            pieces = back[index * ways : (index + 1) * ways]
            extra_in = (weight_raw, *parts) if last else ()
            extra_out = [struct(width, cols, dtype=f32)] + [
                struct(*shape, dtype=f32) for shape in ((1, HEAD_DIM), (1, HEAD_DIM), (1, 1))
            ]
            outs = run(
                functools.partial(
                    unpack_body,
                    ways=ways,
                    width=width,
                    start=index * size,
                    size=size,
                    finish=len(parts) if last else 0,
                ),
                [struct(rows, features)] * 3 + (extra_out if last else []),
                (places, *pieces, *extra_in, *outs),
                [SMEM] + [VMEM] * (ways + len(extra_in)) + [ANY] * len(outs),
                [ANY] * 3 + [VMEM] * (4 if last else 0),
                [pltpu.SemaphoreType.DMA((ways, 3))],
                room=2 * size_of(*pieces) + (8 * width * lanes if last else 0),
                alias={1 + ways + len(extra_in) + i: i for i in range(len(outs))},
            )
        *grads, weight_grad, q_gain, k_gain, norm = outs
        return (
            *[grad[None] for grad in grads],
            weight_grad,
            q_gain[0],
            k_gain[0],
            norm[0, 0],
        )

    return local


def solution(mesh):
    rows = P("dp", "seq", None)
    groups, ways = mesh.shape["dp"], mesh.shape["seq"]
    body = make_local(groups, ways)

    return jax.shard_map(
        body,
        mesh=mesh,
        in_specs=(rows, rows, rows, rows, P("dp", None), P("seq", None), P(), P()),
        out_specs=(rows, rows, rows, P("seq", "dp"), P(), P(), P()),
        check_vma=False,
    )
```

```python
import functools
import math
import jax
import jax.numpy as jnp
from jax import lax
from jax.experimental import pallas as pl
from jax.experimental.pallas import tpu as pltpu
from jax.sharding import PartitionSpec as P

HEAD_DIM = 128
MAX_NORM = 768
EPS = 1e-06
CORES = 2
CHUNKS = 2
HALVES = 2
TOGETHER = 3
MIB = 1024 * 1024


ANY = pl.BlockSpec(memory_space=pl.ANY)
SMEM = pl.BlockSpec(memory_space=pltpu.SMEM)
VMEM = pl.BlockSpec(memory_space=pltpu.VMEM)


def run(body, outs, args, in_specs, out_specs, scratch=(), grid=None, room=0, alias=None):
    return pl.pallas_call(
        body,
        out_shape=outs,
        grid=() if grid is None else grid,
        in_specs=in_specs,
        out_specs=out_specs,
        scratch_shapes=list(scratch),
        input_output_aliases=alias or {},
        compiler_params=pltpu.CompilerParams(vmem_limit_bytes=min(room + 4 * MIB, 62 * MIB)),
    )(*args)


def size_of(*arrays):
    return sum(math.prod(x.shape) * x.dtype.itemsize for x in arrays)


def chunk_count(heads):
    return max(c for c in range(1, CHUNKS + 1) if heads % c == 0)


def dot(a, b, dims=(1, 0)):
    contract = (((dims[0],), (dims[1],)), ((), ()))
    return lax.dot_general(a, b, contract, preferred_element_type=jnp.float32)


def pack_body(place_ref, *refs, ways, width):
    rows, outs = refs[:3], refs[3:]
    place = place_ref[0]
    for step in range(ways):
        column = pl.multiple_of(lax.rem(place + step, ways) * width, 128)
        for which in range(3):
            outs[step][which] = rows[which][:, pl.ds(column, width)]


def unpack_body(place_ref, *refs, ways, width, start, size, finish, early_steps):
    early = dict(zip(early_steps, refs))
    refs = refs[len(early_steps) :]
    pieces, sems = refs[:ways], refs[-1]
    place = place_ref[0]
    outs = refs[-8:-5] if finish else refs[-4:-1]
    copies = []
    for step, piece in enumerate(pieces):
        column = pl.multiple_of(lax.rem(place_ref[0] + step, ways) * width + start, 128)
        for which in range(3):
            target = outs[which].at[:, pl.ds(column, size)]
            copy = pltpu.make_async_copy(piece.at[which], target, sems.at[step, which])
            copies.append(copy)
            if step not in early:
                copy.start()
                continue
            source = early[step].at[which, :, start : start + size]
            other = pltpu.make_async_copy(source, target, sems.at[step, which])
            late = jnp.logical_or(at_end(place, ways), at_end(lax.rem(place + step, ways), ways))
            pl.when(late)(copy.start)
            pl.when(jnp.logical_not(late))(other.start)
    if finish:
        grad_ref, q_ref, k_ref, norm_ref = refs[-5:-1]
        weight_ref, parts = refs[ways], refs[ways + 1 : ways + 1 + finish]
        total = sum(part[...] for part in parts)
        q_gain, k_gain = total[0:1], total[1:2]
        squares = total[2:3] + q_gain * q_gain + k_gain * k_gain
        norm = jnp.sqrt(jnp.sum(squares, axis=1, keepdims=True))
        factor = jnp.minimum(jnp.float32(1.0), MAX_NORM / (norm + EPS))
        grad_ref[...] = weight_ref[...] * factor
        q_ref[...] = q_gain * factor
        k_ref[...] = k_gain * factor
        norm_ref[...] = norm
    for copy in copies:
        copy.wait()


def at_end(place, ways):
    return jnp.logical_or(place == 0, place == ways - 1)


def item_of(place, index, ways):
    both = jnp.minimum(place, ways - 1 - place)
    paired = index <= 2 * both
    hops = jnp.where(paired, (index + 1) // 2, index - both)
    lefty = jnp.where(paired, index % 2 == 1, 2 * place > ways - 1)
    return hops, lefty


def slot_of(place, index, ways):
    if index == 0:
        return jnp.int32(0)
    hops, lefty = item_of(place, index, ways)
    return jnp.where(lefty, hops, ways - hops)


def d_attn_body(place_ref, *refs, index, ways, groups, hops_list, parts, rows, cols, aligned, span, emit, when):
    count = sum(parts) * (2 if index else 1)
    sources, weight = refs[:count], refs[count]
    outs, full = refs[count + 1 : -1], refs[-1]
    place, group = place_ref[0], place_ref[1]

    def take(pieces):
        height = rows // len(pieces)
        for i, piece in enumerate(pieces):
            full[i * height : (i + 1) * height, :] = piece[...]

    if index == 0:
        take(sources)
    else:
        if when == "early":
            take(sources[: parts[0]])
        hops, lefty = item_of(place, index, ways)
        at = 0
        for dist, number in zip(hops_list, parts):
            for side in range(2):
                here = jnp.logical_and(hops == dist, lefty == (side == 0))
                pl.when(here)(functools.partial(take, sources[at : at + number]))
                at += number


    def multiply():
        part = weight[span[0] : span[1], :]
        outs[0][...] = dot(full[...], part, (1, 1)).astype(jnp.bfloat16)

    if when == "late":
        pl.when(at_end(place, ways))(multiply)
    else:
        multiply()
    if not emit:
        return
    if aligned:
        for mask in range(groups):
            column = pl.multiple_of(lax.bitwise_xor(group, mask) * cols, 128)
            outs[1 + mask][...] = full[:, pl.ds(column, cols)]
    else:
        outs[1][...] = full[...]


def segments(place, lengths_ref, shape, dim, ways, rows):
    index = lax.broadcasted_iota(jnp.int32, shape, dim)
    source = place - lax.div(index, rows)
    source = jnp.where(source < 0, source + ways, source)
    position = source * rows + lax.rem(index, rows)
    seg = jnp.zeros(shape, jnp.int32)
    end = jnp.int32(0)
    for clip in range(lengths_ref.shape[1]):
        end = end + lengths_ref[0, clip]
        seg = seg + (position >= end).astype(jnp.int32)
    return seg


def norm_rows(raw, gain):
    wide = raw.astype(jnp.float32)
    inverse = lax.rsqrt(jnp.mean(wide * wide, axis=-1, keepdims=True) + EPS)
    unit = wide * inverse
    return unit, inverse, (unit * gain).astype(jnp.bfloat16)


def norm_back(unit, inverse, gain, d_norm):
    d_unit = d_norm * gain
    grad = inverse * (d_unit - unit * jnp.mean(unit * d_unit, axis=-1, keepdims=True))
    return grad.astype(jnp.bfloat16), jnp.sum(unit * d_norm, axis=0, keepdims=True)


def forward_body(place_ref, lengths_ref, *refs, ways, rows):
    pieces = refs[:ways]
    q_gain_ref, k_gain_ref, attn_t_ref, probs_ref = refs[ways:]
    total = ways * rows
    place = place_ref[0]
    scale = HEAD_DIM ** (-0.5)
    same = segments(place, lengths_ref, (total, 1), 0, ways, rows) == segments(
        place, lengths_ref, (1, total), 1, ways, rows
    )

    def gather(which):
        return jnp.concatenate([piece[which] for piece in pieces], axis=0)

    _, _, q_norm = norm_rows(gather(0), q_gain_ref[...])
    _, _, k_norm = norm_rows(gather(1), k_gain_ref[...])
    value = gather(2)
    scores = dot(k_norm, q_norm, (1, 1)) * scale
    expo = jnp.where(same, jnp.exp(scores), 0.0)
    inverse_sum = 1.0 / jnp.sum(expo, axis=0, keepdims=True)
    probs = (expo * inverse_sum).astype(jnp.bfloat16)
    probs_ref[0] = probs
    attn_t_ref[...] = dot(value.T, probs).astype(jnp.bfloat16)


def backward_body(place_ref, *refs, late, index, ways, **sizes):
    if not late:
        backward_rows(place_ref, refs, ways, **sizes)
        return
    before, rest = refs[: ways + 1], refs[ways + 1 :]
    end = at_end(place_ref[0], ways)

    @pl.when(end)
    def _():
        backward_rows(place_ref, rest, ways, **sizes)

    @pl.when(jnp.logical_not(end))
    def _():
        outs = rest[2 * ways + 3 : -1]
        outs[0][...] = before[0][...] if index == 0 else jnp.zeros_like(outs[0])
        for step in range(ways):
            outs[1 + step][...] = before[1 + step][...]


def backward_rows(place_ref, refs, ways, rows, heads):
    pieces = refs[:ways]
    d_pieces = refs[ways : 2 * ways]
    probs_ref, q_gain_ref, k_gain_ref, gains_ref = refs[2 * ways : 2 * ways + 4]
    outs = refs[2 * ways + 4 : 3 * ways + 4]
    d_attn_ref = refs[-1]
    place = place_ref[0]
    scale = HEAD_DIM ** (-0.5)
    for index in range(ways):
        row = pl.multiple_of(slot_of(place, index, ways) * rows, rows)
        d_attn_ref[pl.ds(row, rows), :] = d_pieces[index][...]
    q_gain = q_gain_ref[...]
    k_gain = k_gain_ref[...]
    q_sum = jnp.zeros((1, HEAD_DIM), jnp.float32)
    k_sum = jnp.zeros((1, HEAD_DIM), jnp.float32)
    for head in range(heads):
        part = slice(head * HEAD_DIM, (head + 1) * HEAD_DIM)

        def gather(which):
            return jnp.concatenate([piece[which, :, part] for piece in pieces], axis=0)

        q_unit, q_inv, q_norm = norm_rows(gather(0), q_gain)
        k_unit, k_inv, k_norm = norm_rows(gather(1), k_gain)
        value = gather(2)
        d_attn = d_attn_ref[:, part]
        probs = probs_ref[head]
        d_probs = dot(value, d_attn, (1, 1))
        probs32 = probs.astype(jnp.float32)
        row_sum = jnp.sum(probs32 * d_probs, axis=0, keepdims=True)
        d_scores = (probs32 * (d_probs - row_sum) * scale).astype(jnp.bfloat16)
        d_value = dot(probs, d_attn).astype(jnp.bfloat16)
        d_k = dot(d_scores, q_norm)
        d_q = dot(k_norm.T, d_scores).T
        q_grad, q_part = norm_back(q_unit, q_inv, q_gain, d_q)
        k_grad, k_part = norm_back(k_unit, k_inv, k_gain, d_k)
        q_sum = q_sum + q_part
        k_sum = k_sum + k_part
        for step in range(ways):
            block = slice(step * rows, (step + 1) * rows)
            outs[step][0, :, part] = q_grad[block]
            outs[step][1, :, part] = k_grad[block]
            outs[step][2, :, part] = d_value[block]
    gains_ref[...] = jnp.concatenate(
        [q_sum, k_sum, jnp.zeros((6, HEAD_DIM), jnp.float32)], axis=0
    )


def weight_body(place_ref, *refs, items, ways, groups, rows, first, last):
    attn = refs[:groups]
    columns = refs[groups : (1 + len(items)) * groups]
    outs = refs[-2:] if last else refs[-1:]
    gain_refs = refs[(1 + len(items)) * groups + 1 : -2]
    left = []
    for index in items:
        slot = pl.multiple_of(slot_of(place_ref[0], index, ways) * rows, 128)
        left += [piece[:, pl.ds(slot, rows)] for piece in attn]
    right = [piece[...] for piece in columns]
    total = dot(jnp.concatenate(left, axis=1), jnp.concatenate(right, axis=0))
    if not first:
        total = total + refs[(1 + len(items)) * groups][...]
    outs[0][...] = total
    if last:
        squares = jnp.sum(jnp.sum(total * total, axis=0, keepdims=True), axis=1, keepdims=True)
        gains = sum(ref[...] for ref in gain_refs)
        row = lax.broadcasted_iota(jnp.int32, gains.shape, 0)
        outs[1][...] = gains + jnp.where(row == 2, squares / HEAD_DIM, 0.0)


def weight_items(ways):
    count = ways - 1
    starts = range(0, count, TOGETHER)
    return [list(range(i, min(i + TOGETHER, count))) for i in starts] + [[count]]


def make_local(groups, ways):
    def local(
        query_rows, key_rows, value_rows, out_grad, clip_lengths, out_weight, query_gain, key_gain
    ):
        place = lax.axis_index("seq")
        group = lax.axis_index("dp")
        places = jnp.stack([place, group]).astype(jnp.int32)
        rows, features = query_rows.shape[1:]
        width = features // ways
        heads = width // HEAD_DIM
        count = chunk_count(heads)
        size = width // count
        model = out_grad.shape[2]
        cols = model // groups
        aligned = cols % 128 == 0
        total = ways * rows
        bf16 = jnp.bfloat16
        f32 = jnp.float32
        lanes = -(-cols // 128) * 128

        def struct(*shape, dtype=bf16):
            return jax.ShapeDtypeStruct(shape, dtype)

        def shift(x, step):
            return lax.ppermute(x, "seq", [(i, (i + step) % ways) for i in range(ways)])

        def partner(x, mask):
            return lax.ppermute(x, "dp", [(i, i ^ mask) for i in range(groups)])

        packed = run(
            functools.partial(pack_body, ways=ways, width=width),
            [struct(3, rows, width)] * ways,
            (places, query_rows[0], key_rows[0], value_rows[0]),
            [SMEM, VMEM, VMEM, VMEM],
            [VMEM] * ways,
            room=6 * size_of(query_rows),
        )
        pieces = [packed[0]] + [shift(packed[step], step) for step in range(1, ways)]

        extra = [struct(rows, cols)] * groups if aligned else [struct(rows, model)]
        right, left = [[out_grad[0]]], [[out_grad[0]]]
        d_attn, columns = [], []
        for index in range(ways):
            if index > 0:
                up = [(i, i + 1) for i in range(index - 1, ways - 1)]
                down = [(i, i - 1) for i in range(1, ways - index + 1)]
                if index == 2:
                    part = rows // HALVES
                    sent = [
                        [side[1][0][half * part : (half + 1) * part] for half in range(HALVES)]
                        for side in (right, left)
                    ]
                else:
                    sent = [right[-1], left[-1]]
                right.append([])
                left.append([])
                for half in range(len(sent[0])):
                    right[-1].append(lax.ppermute(sent[0][half], "seq", up))
                    left[-1].append(lax.ppermute(sent[1][half], "seq", down))
            hops_list = list(range((index + 1) // 2, index + 1)) if index else [0]
            sources = [x for dist in hops_list for side in (right, left) for x in side[dist]]
            if index == 0:
                sources = [out_grad[0]]

            def piece(span, emit, when="", hops_list=hops_list, sources=sources):
                return run(
                    functools.partial(
                        d_attn_body,
                        index=index,
                        ways=ways,
                        groups=groups,
                        hops_list=hops_list,
                        parts=[len(right[dist]) for dist in hops_list],
                        rows=rows,
                        cols=cols,
                        aligned=aligned,
                        span=span,
                        emit=emit,
                        when=when,
                    ),
                    [struct(rows, span[1] - span[0])] + (extra if emit else []),
                    (places, *sources, out_weight),
                    [SMEM] + [VMEM] * (len(sources) + 1),
                    [VMEM] * (1 + (len(extra) if emit else 0)),
                    [pltpu.VMEM((rows, model), bf16)],
                    room=size_of(out_weight, out_grad, out_grad, *sources),
                )

            lead = []
            if index == ways - 1:
                near = hops_list[:-1]
                have = [x for dist in near for side in (right, left) for x in side[dist]]
                early_piece = piece((0, size), False, "early", near, have)[0]
                if count > 1:
                    lead = piece((0, size), False, "late")
            results = piece((size if lead else 0, width), True)
            d_attn.append((*lead, results[0]))
            blocks = results[1:]
            if not aligned:
                blocks = [
                    lax.dynamic_slice_in_dim(results[1], (group ^ mask) * cols, cols, 1)
                    for mask in range(groups)
                ]
            got = {mask: partner(blocks[mask], mask) for mask in reversed(range(1, groups))}
            columns.append([blocks[0]] + [got[mask] for mask in range(1, groups)])

        attn_t, probs = run(
            functools.partial(forward_body, ways=ways, rows=rows),
            [struct(width, total), struct(heads, total, total)],
            (places, clip_lengths, *pieces, query_gain[None], key_gain[None]),
            [SMEM, SMEM]
            + [pl.BlockSpec((3, rows, HEAD_DIM), lambda h: (0, 0, h))] * ways
            + [pl.BlockSpec((1, HEAD_DIM), lambda h: (0, 0))] * 2,
            [
                pl.BlockSpec((HEAD_DIM, total), lambda h: (h, 0)),
                pl.BlockSpec((1, total, total), lambda h: (h, 0, 0)),
            ],
            grid=(heads,),
            room=24 * total * total + 4 * MIB,
        )
        attn = [attn_t]
        for mask in range(1, groups):
            if mask % CORES:
                attn.append(partner(attn[mask - 1], 1))
            else:
                attn.append(partner(attn_t, mask))

        def backward(index, size, late, d_pieces, before):
            row_spec = pl.BlockSpec((3, rows, size), lambda i: (0, 0, index))
            gain_specs = [pl.BlockSpec((1, HEAD_DIM), lambda i: (0, 0))] * 2
            sum_spec = pl.BlockSpec((8, HEAD_DIM), lambda i: (0, 0))
            return run(
                functools.partial(
                    backward_body,
                    late=late,
                    index=index,
                    ways=ways,
                    rows=rows,
                    heads=size // HEAD_DIM,
                ),
                [struct(8, HEAD_DIM, dtype=f32)] + [struct(3, rows, size)] * ways,
                (
                    places,
                    *before,
                    *pieces,
                    *[x for x, _ in d_pieces],
                    probs,
                    query_gain[None],
                    key_gain[None],
                ),
                [SMEM]
                + ([sum_spec] + [row_spec] * ways if late else [])
                + [row_spec] * ways
                + [pl.BlockSpec((rows, size), lambda i, b=b: (0, b)) for _, b in d_pieces]
                + [pl.BlockSpec((size // HEAD_DIM, total, total), lambda i: (index, 0, 0))]
                + gain_specs,
                [sum_spec] + [pl.BlockSpec((3, rows, size), lambda i: (0, 0, 0))] * ways,
                [pltpu.VMEM((total, size), bf16)],
                grid=(1,),
                room=(20 + 4 * (size // HEAD_DIM)) * total * total
                + 8 * MIB
                + 2 * size_of(*pieces) * size // width,
            )

        before = backward(
            0, size, False, [(x[-1], 0) for x in d_attn[:-1]] + [(early_piece, 0)], ()
        )
        inner = range(1, ways - 1)
        early, late_pairs = {}, {}
        for step in range(1, ways):
            pairs = [(i, (i - step) % ways) for i in range(ways)]
            near = [pair for pair in pairs if pair[0] in inner and pair[1] in inner]
            late_pairs[step] = [pair for pair in pairs if pair not in near]
            if near:
                early[step] = lax.ppermute(before[1 + step], "seq", near)

        gains = []
        back = []
        for index in range(count):
            d_pieces = [
                (x[-1 if index else 0], max(0, index + 1 - len(x))) for x in d_attn
            ]
            results = backward(index, size, index == 0, d_pieces, () if index else before)
            gains.append(results[0])
            grads = results[1:]
            back.append(grads[0])
            for step in range(1, ways):
                if index == 0:
                    back.append(lax.ppermute(grads[step], "seq", late_pairs[step]))
                else:
                    back.append(shift(grads[step], -step))

        weight_raw = None
        for items in weight_items(ways):
            first, last = weight_raw is None, items[-1] == ways - 1
            results = run(
                functools.partial(
                    weight_body,
                    items=items,
                    ways=ways,
                    groups=groups,
                    rows=rows,
                    first=first,
                    last=last,
                ),
                [struct(width, cols, dtype=f32)]
                + ([struct(8, HEAD_DIM, dtype=f32)] if last else []),
                (places, *attn)
                + tuple(x for index in items for x in columns[index])
                + (() if first else (weight_raw,))
                + (tuple(gains) if last else ()),
                [SMEM]
                + [VMEM]
                * ((1 + len(items)) * groups + (0 if first else 1) + (len(gains) if last else 0)),
                [VMEM] * (2 if last else 1),
                room=groups * (total * width + len(items) * rows * (lanes + width)) * 2
                + 12 * width * lanes,
            )
            weight_raw = results[0]

        parts = [results[1]]
        for axis, number in (("dp", groups), ("seq", ways)):
            mask = 1
            while mask < number:
                radix = 4 if mask * 4 <= number and (axis == "seq" or mask > 1) else 2
                sent = sum(parts[1:], parts[0])
                parts = [sent]
                for step in range(1, radix):
                    if axis == "dp":
                        parts.append(partner(sent, mask * step))
                    else:
                        aside = 0
                        pairs = [
                            (d * ways + i, (d ^ aside) * ways + (i ^ (mask * step)))
                            for d in range(groups)
                            for i in range(ways)
                        ]
                        parts.append(lax.ppermute(sent, ("dp", "seq"), pairs))
                mask *= radix
        outs = ()
        for index in range(count):
            last = index == count - 1
            inner_rows = early if index == 0 else {}
            pieces = back[index * ways : (index + 1) * ways]
            extra_in = (weight_raw, *parts) if last else ()
            extra_out = [struct(width, cols, dtype=f32)] + [
                struct(*shape, dtype=f32) for shape in ((1, HEAD_DIM), (1, HEAD_DIM), (1, 1))
            ]
            outs = run(
                functools.partial(
                    unpack_body,
                    ways=ways,
                    width=width,
                    start=index * size,
                    size=size,
                    finish=len(parts) if last else 0,
                    early_steps=list(inner_rows),
                ),
                [struct(rows, features)] * 3 + (extra_out if last else []),
                (places, *inner_rows.values(), *pieces, *extra_in, *outs),
                [SMEM] + [VMEM] * (len(inner_rows) + ways + len(extra_in)) + [ANY] * len(outs),
                [ANY] * 3 + [VMEM] * (4 if last else 0),
                [pltpu.SemaphoreType.DMA((ways, 3))],
                room=2 * size_of(*pieces, *inner_rows.values()) + (8 * width * lanes if last else 0),
                alias={1 + len(inner_rows) + ways + len(extra_in) + i: i for i in range(len(outs))},
            )
        *grads, weight_grad, q_gain, k_gain, norm = outs
        return (
            *[grad[None] for grad in grads],
            weight_grad,
            q_gain[0],
            k_gain[0],
            norm[0, 0],
        )

    return local


def solution(mesh):
    rows = P("dp", "seq", None)
    groups, ways = mesh.shape["dp"], mesh.shape["seq"]
    body = make_local(groups, ways)

    return jax.shard_map(
        body,
        mesh=mesh,
        in_specs=(rows, rows, rows, rows, P("dp", None), P("seq", None), P(), P()),
        out_specs=(rows, rows, rows, P("seq", "dp"), P(), P(), P()),
        check_vma=False,
    )
```
